256 devices in a mesh: row: 16 (over z_lo, y), col: 16 (over z_hi, x, core).
Axes of the slice: x: 4, y: 4, z: 8 (z_hi: 2, z_lo: 4; z = z_hi * 4 + z_lo), core: 2. Of those that a mesh axis runs over, the one named last changes fastest.
Arguments:
- orbitals: float32 [2048, 28672], P(('row', 'col')), may hold values from -0.03125 to 0.03125
- applied: float32 [2048, 28672], P(('row', 'col')), may hold values from -24 to 24
Outputs:
- hamiltonian: float32 [2048, 2048], P('col', 'row')
- intersection: float32 [2048, 2048], P('col', 'row')
The draws below stay inside these ranges and needn't reach their ends.
All inputs are finite; a program needn't handle non-finite values.
Results may differ from the reference program's by a relative error of at most 0.000098.
Values sent between devices are 32-bit elements; how exact they have to be, the bound alone decides.
A program may use at most 64 MiB of HBM per device.

```python
import jax
import jax.numpy as jnp
from jax import lax

NORB = 2048
NCOEF = 28672


def strengthened(values, stream_key, source, target, shards_of, factor):
    def block_of(dim):
        return (jnp.arange(values.shape[dim]) // (values.shape[dim] // shards_of)).reshape((-1,) + (1,) * (values.ndim - 1 - dim))

    near = jax.random.permutation(stream_key, shards_of)[block_of(target)]
    other_side = (block_of(target) + shards_of // 2) % shards_of
    return jnp.where((block_of(source) == near) | (block_of(source) == other_side), factor * values, values)


def block_scale(rng, extent, pieces, smallest, largest):
    gain, own = 1.0, jax.random.fold_in(rng, 6)
    for position, parts in pieces:
        steps = jnp.exp(jax.random.uniform(jax.random.fold_in(own, position), (parts,), jnp.float32, smallest / len(pieces), largest / len(pieces)))
        gain = gain * jnp.repeat(steps, extent[position] // parts).reshape([-1 if axis == position else 1 for axis in range(len(extent))])
    return gain


def noise(key, dims, spread, bound, split=(), dtype=jnp.bfloat16):
    level = block_scale(key, dims, split, -0.22, 0.18) if split else 1.0
    values = jax.random.normal(key, dims, jnp.float32) * spread * level
    return jnp.minimum(jnp.maximum(values, -bound), bound).astype(dtype)


def noise_with(stream_key, extent, deviation, most, pieces, heavy, dtype=jnp.bfloat16):
    drawn = deviation * jax.random.normal(stream_key, extent, jnp.float32)
    if pieces:
        drawn = drawn * block_scale(stream_key, extent, pieces, -0.22, 0.18)
    return jnp.clip(strengthened(drawn, jax.random.fold_in(stream_key, 3), *heavy), -most, most).astype(dtype)


def setup_inputs(seed: int = 0) -> dict:
    key_of = jax.random.split(jax.random.key(seed), 3)
    return {
        "orbitals": noise(key_of[0], (NORB, NCOEF), NCOEF ** -0.5, 0.03125, ((0, 256),), jnp.float32),
        "applied": noise_with(key_of[1], (NORB, NCOEF), 1.0, 24.0, ((0, 256),), (1, 0, 256, 6.0), jnp.float32),
    }


def reference(orbitals, applied):
    hamiltonian = jnp.dot(orbitals, applied.T, precision=lax.Precision.HIGHEST, preferred_element_type=jnp.float32)
    intersection = jnp.dot(orbitals, orbitals.T, precision=lax.Precision.HIGHEST, preferred_element_type=jnp.float32)
    return hamiltonian, intersection
```

```python
import jax
import jax.numpy as jnp
from jax import lax
from jax.sharding import Mesh, PartitionSpec as P

PLANE = ("zl", "zh", "x", "core")


def halves(a):
    hi = lax.reduce_precision(a, 8, 7)
    lo = a - hi
    return hi.astype(jnp.bfloat16), lo.astype(jnp.bfloat16)


def product(left, right):
    def dot(a, b):
        return lax.dot_general(
            a, b, (((1,), (1,)), ((), ())), preferred_element_type=jnp.float32
        )

    (lh, ll), (rh, rl) = halves(left), halves(right)
    return dot(lh, rh) + (dot(lh, rl) + dot(ll, rh))


def shards(orbitals, applied):
    orb = lax.all_to_all(orbitals, PLANE, split_axis=1, concat_axis=0, tiled=True)
    app = lax.all_to_all(applied, PLANE, split_axis=1, concat_axis=0, tiled=True)
    every = lax.all_gather(orb, "y", axis=0, tiled=False)
    k = orb.shape[1]
    every = every.reshape(4, 4, 128, k).transpose(1, 0, 2, 3).reshape(2048, k)
    parts = product(every, jnp.concatenate([orb, app], axis=0))
    parts = parts.reshape(16, 128, 2, 4, 128).transpose(3, 0, 2, 1, 4)
    parts = parts.reshape(64, 2, 128, 128)
    mine = lax.psum_scatter(parts, PLANE, scatter_dimension=0, tiled=True)
    return mine[0, 1], mine[0, 0]


def solution(mesh):
    fine = Mesh(mesh.devices.reshape(4, 4, 2, 4, 2), ("zl", "y", "zh", "x", "core"))
    placed = (P(("zl", "y", "zh", "x", "core"), None),) * 2
    out = P(("zh", "x", "core"), ("zl", "y"))
    return jax.shard_map(
        shards, mesh=fine, in_specs=placed, out_specs=(out, out), check_vma=False
    )
```

```python
import jax
import jax.numpy as jnp
from jax import lax
from jax.experimental import pallas as pl
from jax.experimental.pallas import tpu as pltpu
from jax.sharding import PartitionSpec as P

MESH = pl.DeviceIdType.MESH
DEPTH = 896
div, rem = lax.div, lax.rem


def drain(ref, sem):
    pltpu.make_async_copy(ref, ref, sem).wait()


def offset_at(t):
    odd = rem(t, 2)
    return odd * div(t + 1, 2) + (1 - odd) * rem(8 - div(t, 2), 8)


def split3(value, low_at):
    hi = value.astype(jnp.bfloat16)
    lo = (value - hi.astype(jnp.float32)).astype(jnp.bfloat16)
    return [lo if n == low_at else hi for n in range(3)]


def kernel(
    orb_hbm, app_hbm, ham_ref, ovl_ref,
    inp, orb, app, left, right, part, xbuf, red, zbuf,
    in_sem, loc_sem, a_send, a_recv, y_send, y_recv, d_send, d_recv,
    x_send, x_recv, z_send, z_recv,
):
    row, col = lax.axis_index("row"), lax.axis_index("col")
    zl, y = div(row, 4), rem(row, 4)
    zh, x, s = div(col, 8), rem(div(col, 2), 4), rem(col, 2)
    z = zh * 4 + zl
    giver = rem(y, 2)
    role_a = s == giver
    role_b = s != giver
    own = div(y, 2)

    def device(zz, yy, xx, ss):
        return (rem(zz, 4) * 4 + yy, div(zz, 4) * 8 + xx * 2 + ss)

    def send(src, dst, send_sem, recv_sem, target):
        pltpu.make_async_remote_copy(
            src_ref=src, dst_ref=dst, send_sem=send_sem, recv_sem=recv_sem,
            device_id=target, device_id_type=MESH,
        ).start()

    sibling = device(z, y, x, 1 - s)
    y_up, y_down = device(z, rem(y + 1, 4), x, s), device(z, rem(y + 3, 4), x, s)
    xr, xl, x2 = rem(x + 1, 4), rem(x + 3, 4), rem(x + 2, 4)

    loads = [
        pltpu.make_async_copy(orb_hbm, inp.at[0], in_sem.at[0]),
        pltpu.make_async_copy(app_hbm, inp.at[1], in_sem.at[1]),
    ]
    for load in loads:
        load.start()

    barrier = pltpu.get_barrier_semaphore()

    def greet(n, carry):
        p = rem(z * 8 + x * 2 + s + n, 64)
        pl.semaphore_signal(
            barrier, inc=1, device_id=device(div(p, 8), y, div(rem(p, 8), 2), rem(p, 2)),
            device_id_type=MESH,
        )
        return carry

    lax.fori_loop(1, 64, greet, 0)
    for target in (y_up, y_down):
        pl.semaphore_signal(barrier, inc=1, device_id=target, device_id_type=MESH)
    for load in loads:
        load.wait()
    pl.semaphore_wait(barrier, 65)

    slot = pl.ds(pl.multiple_of(zl * 128 + col * 8, 8), 8)
    orb_slot, app_slot = orb.at[own, slot], app.at[slot]

    def columns(zz, xx):
        return pl.ds(pl.multiple_of((zz * 4 + xx) * DEPTH, 128), DEPTH)

    def scatter(which, dst, core):
        def step(n, carry):
            d = offset_at(div(n, 4))
            zz, xx = rem(z + d, 8), rem(x + rem(n, 4), 4)
            send(
                inp.at[which, :, columns(zz, xx)], dst, a_send,
                a_recv.at[rem(8 - d, 8)], device(zz, y, xx, core),
            )
            return carry

        lax.fori_loop(1, 32, step, 0)

    orb_mine, app_mine = inp.at[0, :, columns(z, x)], inp.at[1, :, columns(z, x)]

    @pl.when(role_a)
    def _():
        pltpu.make_async_copy(orb_mine, orb_slot, loc_sem).start()

    @pl.when(role_b)
    def _():
        send(orb_mine, orb_slot, a_send, a_recv.at[0], sibling)

    scatter(0, orb_slot, giver)

    @pl.when(role_a)
    def _():
        send(app_mine, app_slot, a_send, a_recv.at[0], sibling)

    @pl.when(role_b)
    def _():
        pltpu.make_async_copy(app_mine, app_slot, loc_sem).start()

    scatter(1, app_slot, 1 - giver)

    def rows_of(t):
        g = offset_at(t)
        zz = rem(z + g, 8)
        return g, pl.multiple_of(rem(zz, 4) * 128 + div(zz, 4) * 64, 64)

    def arrived(t, g):
        @pl.when(t == 0)
        def _():
            drain(app.at[pl.ds(0, 56)], a_recv.at[0])
            drain(app.at[pl.ds(0, 8)], loc_sem)

        @pl.when(t > 0)
        def _():
            drain(app.at[pl.ds(0, 64)], a_recv.at[g])

    @pl.when(role_a)
    def _():
        def pass_on(t, carry):
            g, first = rows_of(t)
            arrived(t, g)
            block = orb.at[own, pl.ds(first, 64)]
            send(block, block, y_send, y_recv.at[0, g], y_up)
            send(block, block, y_send, y_recv.at[1, g], y_down)
            send(block, orb.at[2, pl.ds(first, 64)], d_send, d_recv, sibling)
            return carry

        lax.fori_loop(0, 8, pass_on, 0)

        def take(t, carry):
            for way in range(2):
                drain(app.at[pl.ds(0, 32)], y_recv.at[way, t])
            return carry

        lax.fori_loop(0, 8, take, 0)

    @pl.when(role_b)
    def _():
        below, above = div(rem(y + 3, 4), 2), div(rem(y + 1, 4), 2)

        def pass_on(t, carry):
            g, first = rows_of(t)
            drain(app.at[pl.ds(0, 64)], y_recv.at[0, g])
            low = orb.at[below, pl.ds(first, 32)]
            send(low, low, y_send, y_recv.at[0, g], y_up)
            drain(app.at[pl.ds(0, 64)], y_recv.at[1, g])
            high = orb.at[above, pl.ds(first + 32, 32)]
            send(high, high, y_send, y_recv.at[1, g], y_down)
            return carry

        lax.fori_loop(0, 8, pass_on, 0)
        drain(app, d_recv)

    def set_left(n, carry):
        at = pl.ds(pl.multiple_of(rem(n, 8) * 64, 64), 64)
        for k, piece in enumerate(split3(orb[div(n, 8), at, :], 1)):
            left[div(n, 8), at, k * DEPTH : (k + 1) * DEPTH] = piece
        return carry

    def set_right(read):
        def step(n, carry):
            at = pl.ds(pl.multiple_of(n * 64, 64), 64)
            for k, piece in enumerate(split3(read(at), 2)):
                right[at, k * DEPTH : (k + 1) * DEPTH] = piece
            return carry

        lax.fori_loop(0, 8, step, 0)

    def multiply(mat):
        def step(n, carry):
            plane, tile = div(n, 2), pl.multiple_of(rem(n, 2) * 256, 256)
            part[mat, plane, :, pl.ds(tile, 256)] = lax.dot_general(
                left[plane], right[pl.ds(tile, 256), :],
                (((1,), (1,)), ((), ())), preferred_element_type=jnp.float32,
            )
            return carry

        lax.fori_loop(0, 4, step, 0)

    def block(mat, xd, h):
        first = pl.multiple_of((div(xd, 2) + 2 * h) * 128, 128)
        return part.at[mat, rem(xd, 2), pl.ds(first, 128), :]

    def x_move(mat, kind, xd, h, way):
        send(
            block(mat, xd, h), xbuf.at[way, mat, kind], x_send,
            x_recv.at[way, mat, kind], device(z, y, xr if way == 0 else xl, s),
        )

    def x_wait(way, mat, kind):
        drain(xbuf.at[way, mat, kind], x_recv.at[way, mat, kind])

    def x_first(mat):
        x_move(mat, 0, x2, 0, 0)
        x_move(mat, 0, x2, 1, 1)
        x_move(mat, 1, xr, 1, 0)
        x_move(mat, 1, xl, 0, 1)

    def x_second(mat):
        for way, xd in ((0, xr), (1, xl)):
            x_wait(way, mat, 0)
            mine = block(mat, xd, way)
            mine[...] = mine[...] + xbuf[way, mat, 0]
            x_move(mat, 2, xd, way, way)

    def x_last(mat):
        for way in range(2):
            for kind in (1, 2):
                x_wait(way, mat, kind)
        for h in range(2):
            mine = block(mat, x, h)
            for c in range(4):
                at = slice(c * 128, (c + 1) * 128)
                red[mat, h * 4 + c] = mine[:, at] + (
                    xbuf[0, mat, 2 - h, :, at] + xbuf[1, mat, 1 + h, :, at]
                )

        def step(n, carry):
            zz = rem(z + n, 8)
            send(
                red.at[mat, zz], zbuf.at[mat, 7 - n], z_send, z_recv.at[mat],
                device(zz, y, x, s),
            )
            return carry

        lax.fori_loop(1, 8, step, 0)

    def z_last(mat, out_ref):
        drain(zbuf.at[mat], z_recv.at[mat])
        total = red[mat, z]
        for n in range(7):
            total = total + zbuf[mat, n]
        out_ref[...] = total

    lax.fori_loop(0, 16, set_left, 0)
    mine_at = jnp.where(role_a, own, 2)
    set_right(lambda at: orb[mine_at, at, :])
    multiply(0)
    x_first(0)

    @pl.when(role_b)
    def _():
        def hand_over(t, carry):
            g, first = rows_of(t)
            arrived(t, g)
            piece = app.at[pl.ds(first, 64)]
            send(piece, piece, d_send, d_recv, sibling)
            return carry

        lax.fori_loop(0, 8, hand_over, 0)

    @pl.when(role_a)
    def _():
        drain(app, d_recv)

    set_right(lambda at: app[at, :])
    multiply(1)
    x_second(0)
    x_first(1)
    x_last(0)
    x_second(1)
    x_last(1)
    z_last(0, ovl_ref)
    z_last(1, ham_ref)

    drain(orb.at[0, pl.ds(0, 504)], a_send)

    @pl.when(role_a)
    def _():
        drain(orb.at[pl.ds(0, 2)], y_send)

    @pl.when(role_b)
    def _():
        drain(orb.at[0], y_send)

    drain(app, d_send)
    drain(xbuf, x_send)
    drain(zbuf, z_send)


def shards(orbitals, applied):
    f32, dma = jnp.float32, pltpu.SemaphoreType.DMA
    tile = jax.ShapeDtypeStruct((128, 128), f32)
    ham, ovl = pl.pallas_call(
        kernel,
        out_shape=(tile, tile),
        in_specs=[pl.BlockSpec(memory_space=pl.ANY)] * 2,
        out_specs=(pl.BlockSpec(memory_space=pltpu.VMEM),) * 2,
        scratch_shapes=[
            pltpu.VMEM((2, 8, 28672), f32),
            pltpu.VMEM((3, 512, DEPTH), f32),
            pltpu.VMEM((512, DEPTH), f32),
            pltpu.VMEM((2, 512, 3 * DEPTH), jnp.bfloat16),
            pltpu.VMEM((512, 3 * DEPTH), jnp.bfloat16),
            pltpu.VMEM((2, 2, 512, 512), f32),
            pltpu.VMEM((2, 2, 3, 128, 512), f32),
            pltpu.VMEM((2, 8, 128, 128), f32),
            pltpu.VMEM((2, 7, 128, 128), f32),
            dma((2,)), dma, dma, dma((8,)), dma, dma((2, 8)), dma, dma,
            dma, dma((2, 2, 3)), dma, dma((2,)),
        ],
        compiler_params=pltpu.CompilerParams(
            collective_id=0, has_side_effects=True, vmem_limit_bytes=56 * 1024 * 1024
        ),
    )(orbitals, applied)
    return ham, ovl


def solution(mesh):
    placed = (P(("row", "col"), None),) * 2
    out = P("col", "row")
    return jax.shard_map(
        shards, mesh=mesh, in_specs=placed, out_specs=(out, out), check_vma=False
    )
```

```python
import jax
import jax.numpy as jnp
from jax import lax
from jax.experimental import pallas as pl
from jax.experimental.pallas import tpu as pltpu
from jax.sharding import PartitionSpec as P

MESH = pl.DeviceIdType.MESH
DEPTH = 896
div, rem = lax.div, lax.rem


def drain(ref, sem):
    pltpu.make_async_copy(ref, ref, sem).wait()


def offset_at(t):
    odd = rem(t, 2)
    return odd * div(t + 1, 2) + (1 - odd) * rem(8 - div(t, 2), 8)


def split3(value, low_at):
    hi = value.astype(jnp.bfloat16)
    lo = (value - hi.astype(jnp.float32)).astype(jnp.bfloat16)
    return [lo if n == low_at else hi for n in range(3)]


def kernel(
    orb_hbm, app_hbm, ham_ref, ovl_ref,
    inp, orb, app, left, right, part, xbuf, red, zbuf,
    in_sem, loc_sem, a_send, a_recv, y_send, y_recv, d_send, d_recv,
    x_send, x_recv, z_send, z_recv,
):
    row, col = lax.axis_index("row"), lax.axis_index("col")
    zl, y = div(row, 4), rem(row, 4)
    zh, x, s = div(col, 8), rem(div(col, 2), 4), rem(col, 2)
    z = zh * 4 + zl
    giver = rem(y, 2)
    role_a = s == giver
    role_b = s != giver
    own = div(y, 2)

    def device(zz, yy, xx, ss):
        return (rem(zz, 4) * 4 + yy, div(zz, 4) * 8 + xx * 2 + ss)

    def send(src, dst, send_sem, recv_sem, target):
        pltpu.make_async_remote_copy(
            src_ref=src, dst_ref=dst, send_sem=send_sem, recv_sem=recv_sem,
            device_id=target, device_id_type=MESH,
        ).start()

    sibling = device(z, y, x, 1 - s)
    y_up, y_down = device(z, rem(y + 1, 4), x, s), device(z, rem(y + 3, 4), x, s)
    xr, xl = rem(x + 1, 4), rem(x + 3, 4)

    loads = [
        pltpu.make_async_copy(orb_hbm, inp.at[0], in_sem.at[0]),
        pltpu.make_async_copy(app_hbm, inp.at[1], in_sem.at[1]),
    ]
    for load in loads:
        load.start()

    barrier = pltpu.get_barrier_semaphore()

    def greet(n, carry):
        p = rem(z * 8 + x * 2 + s + n, 64)
        pl.semaphore_signal(
            barrier, inc=1, device_id=device(div(p, 8), y, div(rem(p, 8), 2), rem(p, 2)),
            device_id_type=MESH,
        )
        return carry

    lax.fori_loop(1, 64, greet, 0)
    for target in (y_up, y_down):
        pl.semaphore_signal(barrier, inc=1, device_id=target, device_id_type=MESH)
    for load in loads:
        load.wait()
    pl.semaphore_wait(barrier, 65)

    slot = pl.ds(pl.multiple_of(zl * 128 + col * 8, 8), 8)
    orb_slot, app_slot = orb.at[own, slot], app.at[slot]

    def columns(zz, xx):
        return pl.ds(pl.multiple_of((zz * 4 + xx) * DEPTH, 128), DEPTH)

    def scatter(which, dst, core):
        def step(n, carry):
            d = offset_at(div(n, 4))
            zz, xx = rem(z + d, 8), rem(x + rem(n, 4), 4)
            send(
                inp.at[which, :, columns(zz, xx)], dst, a_send,
                a_recv.at[rem(8 - d, 8)], device(zz, y, xx, core),
            )
            return carry

        lax.fori_loop(1, 32, step, 0)

    orb_mine, app_mine = inp.at[0, :, columns(z, x)], inp.at[1, :, columns(z, x)]

    @pl.when(role_a)
    def _():
        pltpu.make_async_copy(orb_mine, orb_slot, loc_sem).start()

    @pl.when(role_b)
    def _():
        send(orb_mine, orb_slot, a_send, a_recv.at[0], sibling)

    scatter(0, orb_slot, giver)

    @pl.when(role_a)
    def _():
        send(app_mine, app_slot, a_send, a_recv.at[0], sibling)

    @pl.when(role_b)
    def _():
        pltpu.make_async_copy(app_mine, app_slot, loc_sem).start()

    scatter(1, app_slot, 1 - giver)

    def rows_of(t):
        g = offset_at(t)
        zz = rem(z + g, 8)
        return g, pl.multiple_of(rem(zz, 4) * 128 + div(zz, 4) * 64, 64)

    def arrived(t, g):
        @pl.when(t == 0)
        def _():
            drain(app.at[pl.ds(0, 56)], a_recv.at[0])
            drain(app.at[pl.ds(0, 8)], loc_sem)

        @pl.when(t > 0)
        def _():
            drain(app.at[pl.ds(0, 64)], a_recv.at[g])

    def neighbour(way):
        return device(z, y, xr if way == 0 else xl, s)

    below, above = div(rem(y + 3, 4), 2), div(rem(y + 1, 4), 2)

    def pass_own(t, carry):
        g, first = rows_of(t)
        arrived(t, g)
        block = orb.at[own, pl.ds(first, 64)]
        send(block, block, y_send, y_recv.at[0, g], y_up)
        send(block, block, y_send, y_recv.at[1, g], y_down)
        send(block, orb.at[2, pl.ds(first, 64)], d_send, d_recv, sibling)
        return carry

    def pass_others(t):
        g, first = rows_of(t)
        drain(app.at[pl.ds(0, 64)], y_recv.at[0, g])
        low = orb.at[below, pl.ds(first, 32)]
        send(low, low, y_send, y_recv.at[0, g], y_up)
        drain(app.at[pl.ds(0, 64)], y_recv.at[1, g])
        high = orb.at[above, pl.ds(first + 32, 32)]
        send(high, high, y_send, y_recv.at[1, g], y_down)

    def take(t):
        g, _ = rows_of(t)
        for way in range(2):
            drain(app.at[pl.ds(0, 32)], y_recv.at[way, g])

    def hand_over(t):
        g, first = rows_of(t)
        arrived(t, g)
        piece = app.at[pl.ds(first, 64)]
        send(piece, piece, d_send, d_recv, sibling)

    def set_left(t):
        _, first = rows_of(t)
        for q in range(2):
            to = pl.ds(pl.multiple_of((t * 2 + q) * 64, 64), 64)
            for k, piece in enumerate(split3(orb[q, pl.ds(first, 64), :], 1)):
                left[to, k * DEPTH : (k + 1) * DEPTH] = piece

    def set_right(read):
        def step(n, carry):
            at = pl.ds(pl.multiple_of(n * 64, 64), 64)
            for k, piece in enumerate(split3(read(at), 2)):
                right[at, k * DEPTH : (k + 1) * DEPTH] = piece
            return carry

        lax.fori_loop(0, 8, step, 0)

    def multiply(mat, p):
        got = lax.dot_general(
            left[pl.ds(pl.multiple_of(p * 256, 256), 256), :], right[...],
            (((1,), (1,)), ((), ())), preferred_element_type=jnp.float32,
        )
        part[pl.ds(mat * 16 + p * 4, 4)] = got.reshape(4, 64, 512)

    def place(t, q):
        zz = rem(z + offset_at(t), 8)
        zl_t = rem(zz, 4)
        return rem(2 * rem(zl_t, 2) + q + 4 - x, 4), div(zl_t, 2), div(zz, 4)

    def x_move(n, way):
        send(
            part.at[n], xbuf.at[way, n], x_send, x_recv.at[way, n], neighbour(way)
        )

    def x_wait(n, way):
        drain(xbuf.at[way, n], x_recv.at[way, n])

    def x_first(mat, t):
        for q in range(2):
            n = mat * 16 + t * 2 + q
            far, h, _ = place(t, q)
            for way, near in ((0, 1), (1, 3)):

                @pl.when(((far == 2) & (h == way)) | ((far == near) & (h == 1 - way)))
                def _(n=n, way=way):
                    x_move(n, way)

    def x_second(mat, t):
        for q in range(2):
            n = mat * 16 + t * 2 + q
            far, h, _ = place(t, q)
            for way, near in ((0, 1), (1, 3)):

                @pl.when((far == near) & (h == way))
                def _(n=n, way=way):
                    x_wait(n, way)
                    part[n] = part[n] + xbuf[way, n]
                    x_move(n, way)

    def x_last(mat, t):
        for q in range(2):
            n = mat * 16 + t * 2 + q
            far, h, r = place(t, q)

            @pl.when(far == 0)
            def _(n=n, h=h, r=r):
                x_wait(n, 0)
                x_wait(n, 1)
                half = pl.ds(pl.multiple_of(r * 64, 64), 64)
                for c in range(4):
                    at = slice(c * 128, (c + 1) * 128)
                    zz = h * 4 + c
                    red[mat, zz, half] = part[n, :, at] + (
                        xbuf[0, n, :, at] + xbuf[1, n, :, at]
                    )

                    @pl.when(zz != z)
                    def _(zz=zz):
                        send(
                            red.at[mat, zz, half],
                            zbuf.at[mat, rem(z - zz + 8, 8) - 1, half],
                            z_send, z_recv.at[mat], device(zz, y, x, s),
                        )

    def z_last(mat, out_ref):
        drain(zbuf.at[mat], z_recv.at[mat])
        total = red[mat, z]
        for n in range(7):
            total = total + zbuf[mat, n]
        out_ref[...] = total

    def pair(p, action):
        action(2 * p)
        action(2 * p + 1)

    @pl.when(role_a)
    def _():
        lax.fori_loop(0, 8, pass_own, 0)

    @pl.when(role_b)
    def _():
        def step(t, carry):
            pass_others(t)
            return carry

        lax.fori_loop(0, 4, step, 0)
        drain(app, d_recv)

    mine_at = jnp.where(role_a, own, 2)
    set_right(lambda at: orb[mine_at, at, :])

    def overlaps(p, carry):
        @pl.when(role_a)
        def _():
            pair(p, take)

        @pl.when(role_b & (p >= 2))
        def _():
            pair(p, pass_others)

        pair(p, set_left)
        multiply(0, p)
        pair(p, lambda t: x_first(0, t))

        @pl.when(p >= 2)
        def _():
            pair(p - 2, lambda t: x_second(0, t))

        @pl.when(role_b & (p >= 1))
        def _():
            pair(p - 1, hand_over)

        return carry

    lax.fori_loop(0, 4, overlaps, 0)

    @pl.when(role_b)
    def _():
        pair(3, hand_over)

    @pl.when(role_a)
    def _():
        drain(app, d_recv)

    set_right(lambda at: app[at, :])

    def energies(p, carry):
        multiply(1, p)
        pair(p, lambda t: x_first(1, t))

        @pl.when(p < 2)
        def _():
            pair(p + 2, lambda t: x_second(0, t))

        return carry

    lax.fori_loop(0, 4, energies, 0)

    def finish(p, carry):
        pair(p, lambda t: x_last(0, t))
        pair(p, lambda t: x_second(1, t))
        return carry

    lax.fori_loop(0, 4, finish, 0)

    def close(p, carry):
        pair(p, lambda t: x_last(1, t))
        return carry

    lax.fori_loop(0, 4, close, 0)
    z_last(0, ovl_ref)
    z_last(1, ham_ref)

    drain(orb.at[0, pl.ds(0, 504)], a_send)

    @pl.when(role_a)
    def _():
        drain(orb.at[pl.ds(0, 2)], y_send)

    @pl.when(role_b)
    def _():
        drain(orb.at[0], y_send)

    drain(app, d_send)
    drain(xbuf.at[0, pl.ds(0, 24)], x_send)
    drain(zbuf, z_send)


def shards(orbitals, applied):
    f32, dma = jnp.float32, pltpu.SemaphoreType.DMA
    tile = jax.ShapeDtypeStruct((128, 128), f32)
    ham, ovl = pl.pallas_call(
        kernel,
        out_shape=(tile, tile),
        in_specs=[pl.BlockSpec(memory_space=pl.ANY)] * 2,
        out_specs=(pl.BlockSpec(memory_space=pltpu.VMEM),) * 2,
        scratch_shapes=[
            pltpu.VMEM((2, 8, 28672), f32),
            pltpu.VMEM((3, 512, DEPTH), f32),
            pltpu.VMEM((512, DEPTH), f32),
            pltpu.VMEM((1024, 3 * DEPTH), jnp.bfloat16),
            pltpu.VMEM((512, 3 * DEPTH), jnp.bfloat16),
            pltpu.VMEM((32, 64, 512), f32),
            pltpu.VMEM((2, 32, 64, 512), f32),
            pltpu.VMEM((2, 8, 128, 128), f32),
            pltpu.VMEM((2, 7, 128, 128), f32),
            dma((2,)), dma, dma, dma((8,)), dma, dma((2, 8)), dma, dma,
            dma, dma((2, 32)), dma, dma((2,)),
        ],
        compiler_params=pltpu.CompilerParams(
            collective_id=0, has_side_effects=True, vmem_limit_bytes=56 * 1024 * 1024
        ),
    )(orbitals, applied)
    return ham, ovl


def solution(mesh):
    placed = (P(("row", "col"), None),) * 2
    out = P("col", "row")
    return jax.shard_map(
        shards, mesh=mesh, in_specs=placed, out_specs=(out, out), check_vma=False
    )
```

```python
import jax
import jax.numpy as jnp
from jax import lax
from jax.experimental import pallas as pl
from jax.experimental.pallas import tpu as pltpu
from jax.sharding import PartitionSpec as P

MESH = pl.DeviceIdType.MESH
DEPTH = 896
EAGER = 4
div, rem = lax.div, lax.rem


def drain(ref, sem):
    pltpu.make_async_copy(ref, ref, sem).wait()


def offset_at(t):
    odd = rem(t, 2)
    return odd * div(t + 1, 2) + (1 - odd) * rem(8 - div(t, 2), 8)


def split3(value, low_at):
    hi = value.astype(jnp.bfloat16)
    lo = (value - hi.astype(jnp.float32)).astype(jnp.bfloat16)
    return [lo if n == low_at else hi for n in range(3)]


def kernel(
    orb_hbm, app_hbm, ham_ref, ovl_ref,
    inp, orb, app, left, right, part, xbuf, red, zbuf, turned,
    in_sem, loc_sem, a_send, a_recv, y_send, y_recv, d_send, d_recv,
    x_send, x_recv, z_send, z_recv, t_send, t_recv,
):
    row, col = lax.axis_index("row"), lax.axis_index("col")
    zl, y = div(row, 4), rem(row, 4)
    zh, x, s = div(col, 8), rem(div(col, 2), 4), rem(col, 2)
    z = zh * 4 + zl
    giver = rem(y, 2)
    role_a = s == giver
    role_b = s != giver
    own = div(y, 2)

    def turn_of(plane):
        return jnp.where((plane == 3) | ((plane == 2) & (y >= 2)), 1, 0)

    def plane_of(q):
        return rem(s + 2 * q + 4 - y, 4)

    row_plane = plane_of(rem(x, 2))
    tile_at = rem(zl + 8 - (2 * zh + div(x, 2)) - turn_of(row_plane), 4)
    summed = (row_plane == 0) | (tile_at < 2)
    mirror = (col, row)

    def device(zz, yy, xx, ss):
        return (rem(zz, 4) * 4 + yy, div(zz, 4) * 8 + xx * 2 + ss)

    def send(src, dst, send_sem, recv_sem, target):
        pltpu.make_async_remote_copy(
            src_ref=src, dst_ref=dst, send_sem=send_sem, recv_sem=recv_sem,
            device_id=target, device_id_type=MESH,
        ).start()

    sibling = device(z, y, x, 1 - s)
    y_up, y_down = device(z, rem(y + 1, 4), x, s), device(z, rem(y + 3, 4), x, s)
    xr, xl = rem(x + 1, 4), rem(x + 3, 4)

    loads = [
        pltpu.make_async_copy(orb_hbm, inp.at[0], in_sem.at[0]),
        pltpu.make_async_copy(app_hbm, inp.at[1], in_sem.at[1]),
    ]
    for load in loads:
        load.start()

    barrier = pltpu.get_barrier_semaphore()

    def greet(n, carry):
        zz = rem(z + offset_at(7 - n), 8)
        for i in range(8):
            pl.semaphore_signal(
                barrier, inc=1, device_id=(rem(zz, 4) * 4 + y, div(zz, 4) * 8 + i),
                device_id_type=MESH,
            )
        return carry

    @pl.when(row_plane != 0)
    def _():
        pl.semaphore_signal(barrier, inc=1, device_id=mirror, device_id_type=MESH)

    lax.fori_loop(0, 7, greet, 0)
    for i in range(1, 8):
        pl.semaphore_signal(
            barrier, inc=1, device_id=(row, zh * 8 + rem(x * 2 + s + i, 8)),
            device_id_type=MESH,
        )
    for target in (y_up, y_down):
        pl.semaphore_signal(barrier, inc=1, device_id=target, device_id_type=MESH)
    for load in loads:
        load.wait()
    pl.semaphore_wait(barrier, jnp.where(row_plane == 0, 65, 66))

    slot = pl.ds(pl.multiple_of(zl * 128 + col * 8, 8), 8)
    orb_slot, app_slot = orb.at[own, slot], app.at[slot]

    def columns(zz, xx):
        return pl.ds(pl.multiple_of((zz * 4 + xx) * DEPTH, 128), DEPTH)

    def scatter(which, dst, core):
        def step(n, carry):
            d = offset_at(div(n, 4))
            zz, xx = rem(z + d, 8), rem(x + rem(n, 4), 4)
            send(
                inp.at[which, :, columns(zz, xx)], dst, a_send,
                a_recv.at[rem(8 - d, 8)], device(zz, y, xx, core),
            )
            return carry

        lax.fori_loop(1, 32, step, 0)

    orb_mine, app_mine = inp.at[0, :, columns(z, x)], inp.at[1, :, columns(z, x)]

    @pl.when(role_a)
    def _():
        pltpu.make_async_copy(orb_mine, orb_slot, loc_sem).start()

    @pl.when(role_b)
    def _():
        send(orb_mine, orb_slot, a_send, a_recv.at[0], sibling)

    scatter(0, orb_slot, giver)

    @pl.when(role_a)
    def _():
        send(app_mine, app_slot, a_send, a_recv.at[0], sibling)

    @pl.when(role_b)
    def _():
        pltpu.make_async_copy(app_mine, app_slot, loc_sem).start()

    scatter(1, app_slot, 1 - giver)

    def rows_of(t):
        g = offset_at(t)
        zz = rem(z + g, 8)
        return g, pl.multiple_of(rem(zz, 4) * 128 + div(zz, 4) * 64, 64)

    def arrived(t, g):
        @pl.when(t == 0)
        def _():
            drain(app.at[pl.ds(0, 56)], a_recv.at[0])
            drain(app.at[pl.ds(0, 8)], loc_sem)

        @pl.when(t > 0)
        def _():
            drain(app.at[pl.ds(0, 64)], a_recv.at[g])

    def neighbour(way):
        return device(z, y, xr if way == 0 else xl, s)

    below, above = div(rem(y + 3, 4), 2), div(rem(y + 1, 4), 2)

    def half_of(first, way, half):
        return pl.ds(pl.multiple_of(first + 32 * rem(way + half, 2), 32), 32)

    def y_move(t, half):
        g, first = rows_of(t)
        for way, target in ((0, y_up), (1, y_down)):
            block = orb.at[own, half_of(first, way, half)]
            send(block, block, y_send, y_recv.at[way, g, half], target)

    def pass_own(t, carry):
        g, first = rows_of(t)
        arrived(t, g)
        y_move(t, 0)

        @pl.when(t < EAGER)
        def _():
            y_move(t, 1)

        block = orb.at[own, pl.ds(first, 64)]
        send(block, orb.at[2, pl.ds(first, 64)], d_send, d_recv, sibling)
        return carry

    def y_wait(t, half):
        g, _ = rows_of(t)
        for way in range(2):
            drain(app.at[pl.ds(0, 32)], y_recv.at[way, g, half])

    def pass_others(t):
        g, first = rows_of(t)
        for way, plane, target in ((0, below, y_up), (1, above, y_down)):
            drain(app.at[pl.ds(0, 32)], y_recv.at[way, g, 0])
            block = orb.at[plane, half_of(first, way, 0)]
            send(block, block, y_send, y_recv.at[way, g, 0], target)

    def hand_over(t):
        g, first = rows_of(t)
        arrived(t, g)
        piece = app.at[pl.ds(first, 64)]
        send(piece, piece, d_send, d_recv, sibling)

    def set_left(t):
        _, first = rows_of(t)
        for q in range(2):
            to = pl.ds(pl.multiple_of((t * 2 + q) * 64, 64), 64)
            for k, piece in enumerate(split3(orb[q, pl.ds(first, 64), :], 1)):
                left[to, k * DEPTH : (k + 1) * DEPTH] = piece

    def set_right(read):
        def step(n, carry):
            at = pl.ds(pl.multiple_of(n * 64, 64), 64)
            for k, piece in enumerate(split3(read(at), 2)):
                right[at, k * DEPTH : (k + 1) * DEPTH] = piece
            return carry

        lax.fori_loop(0, 8, step, 0)

    def multiply(mat, p):
        got = lax.dot_general(
            left[pl.ds(pl.multiple_of(p * 256, 256), 256), :], right[...],
            (((1,), (1,)), ((), ())), preferred_element_type=jnp.float32,
        )
        for n in range(4):
            t, q = p * 2 + n // 2, n % 2
            _, zl_t, _ = place(t, q)
            for c in range(4):
                e = c if mat else rem(c + 8 - zl_t - turn_of(plane_of(q)), 4)
                part[mat * 16 + p * 4 + n, e] = got[
                    n * 64 : (n + 1) * 64, c * 128 : (c + 1) * 128
                ]

    def place(t, q):
        zz = rem(z + offset_at(t), 8)
        zl_t = rem(zz, 4)
        return rem(2 * rem(zl_t, 2) + q + 4 - x, 4), zl_t, div(zz, 4)

    def spans(mat, q):
        if mat:
            return ((True, 4),)
        whole = plane_of(q) == 0
        return ((whole, 4), (jnp.logical_not(whole), 2))

    def x_move(mat, n, way, count):
        some = pl.ds(0, count)
        send(
            part.at[n, some], xbuf.at[way, n, some], x_send.at[mat],
            x_recv.at[way, n], neighbour(way),
        )

    def x_wait(n, way, count):
        drain(xbuf.at[way, n, pl.ds(0, count)], x_recv.at[way, n])

    def pieces(mat, t, action):
        for q in range(2):
            n = mat * 16 + t * 2 + q
            far, zl_t, r = place(t, q)
            for cond, count in spans(mat, q):
                action(n, q, far, zl_t, r, cond, count)

    def x_first(mat, t):
        def action(n, q, far, zl_t, r, cond, count):
            h = div(zl_t, 2)
            for way, near in ((0, 1), (1, 3)):

                @pl.when(
                    cond & (((far == 2) & (h == way)) | ((far == near) & (h == 1 - way)))
                )
                def _(way=way):
                    x_move(mat, n, way, count)

        pieces(mat, t, action)

    def x_second(mat, t):
        def action(n, q, far, zl_t, r, cond, count):
            for way, near in ((0, 1), (1, 3)):

                @pl.when(cond & (far == near) & (div(zl_t, 2) == way))
                def _(way=way):
                    x_wait(n, way, count)
                    some = pl.ds(0, count)
                    part[n, some] = part[n, some] + xbuf[way, n, some]
                    x_move(mat, n, way, count)

        pieces(mat, t, action)

    def x_last(mat, t):
        def action(n, q, far, zl_t, r, cond, count):
            @pl.when(cond & (far == 0))
            def _():
                x_wait(n, 0, count)
                x_wait(n, 1, count)
                half = pl.ds(pl.multiple_of(r * 64, 64), 64)
                for e in range(count):
                    c = e if mat else rem(zl_t + turn_of(plane_of(q)) + e, 4)
                    zz = div(zl_t, 2) * 4 + c
                    red[mat, zz, half] = part[n, e] + (xbuf[0, n, e] + xbuf[1, n, e])

                    @pl.when(zz != z)
                    def _(zz=zz):
                        send(
                            red.at[mat, zz, half],
                            zbuf.at[mat, rem(z - zz + 8, 8) - 1, half],
                            z_send.at[mat], z_recv.at[mat], device(zz, y, x, s),
                        )

        pieces(mat, t, action)

    def z_sum(mat):
        drain(zbuf.at[mat], z_recv.at[mat])
        total = red[mat, z]
        for n in range(7):
            total = total + zbuf[mat, n]
        return total

    def pair(p, action):
        action(2 * p)
        action(2 * p + 1)

    @pl.when(role_a)
    def _():
        lax.fori_loop(0, 8, pass_own, 0)

        def rest(t, carry):
            y_move(t, 1)
            return carry

        lax.fori_loop(EAGER, 8, rest, 0)

    @pl.when(role_b)
    def _():
        def step(t, carry):
            pass_others(t)
            return carry

        lax.fori_loop(0, 4, step, 0)
        drain(app, d_recv)

    mine_at = jnp.where(role_a, own, 2)
    set_right(lambda at: orb[mine_at, at, :])

    def overlaps(p, carry):
        @pl.when(role_a)
        def _():
            pair(p, lambda t: y_wait(t, 0))

        @pl.when(role_b & (p < 2))
        def _():
            pair(p + 2, pass_others)

        @pl.when(role_b)
        def _():
            pair(p, lambda t: y_wait(t, 1))

        pair(p, set_left)
        multiply(0, p)
        pair(p, lambda t: x_first(0, t))

        @pl.when(p >= 1)
        def _():
            pair(p - 1, lambda t: x_second(0, t))

        @pl.when(role_b & (p >= 1))
        def _():
            pair(p - 1, hand_over)

        return carry

    lax.fori_loop(0, 4, overlaps, 0)

    @pl.when(role_b)
    def _():
        pair(3, hand_over)

    @pl.when(role_a)
    def _():
        drain(app, d_recv)

    set_right(lambda at: app[at, :])

    def energies(p, carry):
        multiply(1, p)

        @pl.when(p < 2)
        def _():
            pair(p, lambda t: x_first(1, t))

        @pl.when(p == 0)
        def _():
            pair(3, lambda t: x_second(0, t))

        return carry

    lax.fori_loop(0, 4, energies, 0)
    pair(0, lambda t: x_last(0, t))
    pair(1, lambda t: x_last(0, t))
    pair(0, lambda t: x_second(1, t))
    pair(2, lambda t: x_first(1, t))
    pair(2, lambda t: x_last(0, t))
    pair(1, lambda t: x_second(1, t))
    pair(3, lambda t: x_first(1, t))
    pair(3, lambda t: x_last(0, t))
    pair(2, lambda t: x_second(1, t))
    pair(0, lambda t: x_last(1, t))
    pair(1, lambda t: x_last(1, t))
    pair(3, lambda t: x_second(1, t))
    pair(2, lambda t: x_last(1, t))

    @pl.when(summed)
    def _():
        total = z_sum(0)
        ovl_ref[...] = total

        @pl.when(row_plane != 0)
        def _():
            turned[0] = total.T
            send(turned.at[0], turned.at[1], t_send, t_recv, mirror)

    pair(3, lambda t: x_last(1, t))
    ham_ref[...] = z_sum(1)

    @pl.when(jnp.logical_not(summed))
    def _():
        drain(turned.at[1], t_recv)
        ovl_ref[...] = turned[1]

    drain(orb.at[0, pl.ds(0, 504)], a_send)

    @pl.when(role_a)
    def _():
        drain(orb.at[pl.ds(0, 2)], y_send)

    @pl.when(role_b)
    def _():
        drain(orb.at[0], y_send)

    drain(app, d_send)

    def x_done(cond, mat, whole_pieces):
        @pl.when(cond)
        def _():
            drain(xbuf.at[0, pl.ds(0, whole_pieces)], x_send.at[mat])

    x_done(role_b, 0, 6)
    x_done(role_a & (rem(x, 2) == own), 0, 8)
    x_done(role_a & (rem(x, 2) != own), 0, 10)
    x_done(True, 1, 12)

    def z_done(cond, mat, halves):
        @pl.when(cond)
        def _():
            drain(xbuf.at[0, 0:halves, 0], z_send.at[mat])

    z_done(row_plane == 0, 0, 14)
    z_done((row_plane != 0) & summed, 0, 6)
    z_done(jnp.logical_not(summed), 0, 8)
    z_done(True, 1, 14)

    @pl.when(summed & (row_plane != 0))
    def _():
        drain(turned.at[0], t_send)


def shards(orbitals, applied):
    f32, dma = jnp.float32, pltpu.SemaphoreType.DMA
    tile = jax.ShapeDtypeStruct((128, 128), f32)
    ham, ovl = pl.pallas_call(
        kernel,
        out_shape=(tile, tile),
        in_specs=[pl.BlockSpec(memory_space=pl.ANY)] * 2,
        out_specs=(pl.BlockSpec(memory_space=pltpu.VMEM),) * 2,
        scratch_shapes=[
            pltpu.VMEM((2, 8, 28672), f32),
            pltpu.VMEM((3, 512, DEPTH), f32),
            pltpu.VMEM((512, DEPTH), f32),
            pltpu.VMEM((1024, 3 * DEPTH), jnp.bfloat16),
            pltpu.VMEM((512, 3 * DEPTH), jnp.bfloat16),
            pltpu.VMEM((32, 4, 64, 128), f32),
            pltpu.VMEM((2, 32, 4, 64, 128), f32),
            pltpu.VMEM((2, 8, 128, 128), f32),
            pltpu.VMEM((2, 7, 128, 128), f32),
            pltpu.VMEM((2, 128, 128), f32),
            dma((2,)), dma, dma, dma((8,)), dma, dma((2, 8, 2)), dma, dma,
            dma((2,)), dma((2, 32)), dma((2,)), dma((2,)), dma, dma,
        ],
        compiler_params=pltpu.CompilerParams(
            collective_id=0, has_side_effects=True, vmem_limit_bytes=56 * 1024 * 1024
        ),
    )(orbitals, applied)
    return pl.pallas_call(
        settle, out_shape=(tile, tile),
        in_specs=[pl.BlockSpec(memory_space=pltpu.VMEM)] * 2,
        out_specs=(pl.BlockSpec(memory_space=pltpu.VMEM),) * 2,
    )(ham, ovl)


def settle(ham_ref, ovl_ref, ham_out, ovl_out):
    ham_out[...] = ham_ref[...]
    ovl_out[...] = ovl_ref[...]


def solution(mesh):
    placed = (P(("row", "col"), None),) * 2
    out = P("col", "row")
    return jax.shard_map(
        shards, mesh=mesh, in_specs=placed, out_specs=(out, out), check_vma=False
    )
```

```python
import jax
import jax.numpy as jnp
from jax import lax
from jax.experimental import pallas as pl
from jax.experimental.pallas import tpu as pltpu
from jax.sharding import PartitionSpec as P

MESH = pl.DeviceIdType.MESH
DEPTH = 896
EAGER = 4
div, rem = lax.div, lax.rem


def drain(ref, sem):
    pltpu.make_async_copy(ref, ref, sem).wait()


def offset_at(t):
    odd = rem(t, 2)
    return odd * div(t + 1, 2) + (1 - odd) * rem(8 - div(t, 2), 8)


def split3(value, low_at):
    hi = value.astype(jnp.bfloat16)
    lo = (value - hi.astype(jnp.float32)).astype(jnp.bfloat16)
    return [lo if n == low_at else hi for n in range(3)]


def kernel(
    orb_hbm, app_hbm, ham_ref, ovl_ref,
    inp, orb, app, left, right, part, xbuf, red, zbuf, turned,
    in_sem, loc_sem, a_send, a_recv, y_send, y_recv, d_send, d_recv,
    x_send, x_recv, z_send, z_recv, t_send, t_recv,
):
    row, col = lax.axis_index("row"), lax.axis_index("col")
    zl, y = div(row, 4), rem(row, 4)
    zh, x, s = div(col, 8), rem(div(col, 2), 4), rem(col, 2)
    z = zh * 4 + zl
    giver = rem(y, 2)
    role_a = s == giver
    role_b = s != giver
    own = div(y, 2)

    def turn_of(plane):
        return jnp.where((plane == 3) | ((plane == 2) & (y >= 2)), 1, 0)

    def plane_of(q):
        return rem(s + 2 * q + 4 - y, 4)

    row_plane = plane_of(rem(x, 2))
    tile_at = rem(zl + 8 - (2 * zh + div(x, 2)) - turn_of(row_plane), 4)
    summed = (row_plane == 0) | (tile_at < 2)
    mirror = (col, row)

    def device(zz, yy, xx, ss):
        return (rem(zz, 4) * 4 + yy, div(zz, 4) * 8 + xx * 2 + ss)

    def send(src, dst, send_sem, recv_sem, target):
        pltpu.make_async_remote_copy(
            src_ref=src, dst_ref=dst, send_sem=send_sem, recv_sem=recv_sem,
            device_id=target, device_id_type=MESH,
        ).start()

    sibling = device(z, y, x, 1 - s)
    y_up, y_down = device(z, rem(y + 1, 4), x, s), device(z, rem(y + 3, 4), x, s)
    xr, xl = rem(x + 1, 4), rem(x + 3, 4)

    loads = [
        pltpu.make_async_copy(orb_hbm, inp.at[0], in_sem.at[0]),
        pltpu.make_async_copy(app_hbm, inp.at[1], in_sem.at[1]),
    ]
    for load in loads:
        load.start()

    barrier = pltpu.get_barrier_semaphore()

    def greet(n, carry):
        zz = rem(z + offset_at(7 - n), 8)
        for i in range(8):
            pl.semaphore_signal(
                barrier, inc=1, device_id=(rem(zz, 4) * 4 + y, div(zz, 4) * 8 + i),
                device_id_type=MESH,
            )
        return carry

    @pl.when(row_plane != 0)
    def _():
        pl.semaphore_signal(barrier, inc=1, device_id=mirror, device_id_type=MESH)

    lax.fori_loop(0, 7, greet, 0)
    for i in range(1, 8):
        pl.semaphore_signal(
            barrier, inc=1, device_id=(row, zh * 8 + rem(x * 2 + s + i, 8)),
            device_id_type=MESH,
        )
    for target in (y_up, y_down):
        pl.semaphore_signal(barrier, inc=1, device_id=target, device_id_type=MESH)
    for load in loads:
        load.wait()
    pl.semaphore_wait(barrier, jnp.where(row_plane == 0, 65, 66))

    slot = pl.ds(pl.multiple_of(zl * 128 + col * 8, 8), 8)
    orb_slot, app_slot = orb.at[own, slot], app.at[slot]

    def columns(zz, xx):
        return pl.ds(pl.multiple_of((zz * 4 + xx) * DEPTH, 128), DEPTH)

    def scatter(which, dst, core):
        def step(n, carry):
            d = offset_at(div(n, 4))
            zz, xx = rem(z + d, 8), rem(x + rem(n, 4), 4)
            send(
                inp.at[which, :, columns(zz, xx)], dst, a_send,
                a_recv.at[rem(8 - d, 8)], device(zz, y, xx, core),
            )
            return carry

        lax.fori_loop(1, 32, step, 0)

    orb_mine, app_mine = inp.at[0, :, columns(z, x)], inp.at[1, :, columns(z, x)]

    @pl.when(role_a)
    def _():
        pltpu.make_async_copy(orb_mine, orb_slot, loc_sem).start()

    @pl.when(role_b)
    def _():
        send(orb_mine, orb_slot, a_send, a_recv.at[0], sibling)

    scatter(0, orb_slot, giver)

    @pl.when(role_a)
    def _():
        send(app_mine, app_slot, a_send, a_recv.at[0], sibling)

    @pl.when(role_b)
    def _():
        pltpu.make_async_copy(app_mine, app_slot, loc_sem).start()

    scatter(1, app_slot, 1 - giver)

    def rows_of(t):
        g = offset_at(t)
        zz = rem(z + g, 8)
        return g, pl.multiple_of(rem(zz, 4) * 128 + div(zz, 4) * 64, 64)

    def arrived(t, g):
        @pl.when(t == 0)
        def _():
            drain(app.at[pl.ds(0, 56)], a_recv.at[0])
            drain(app.at[pl.ds(0, 8)], loc_sem)

        @pl.when(t > 0)
        def _():
            drain(app.at[pl.ds(0, 64)], a_recv.at[g])

    def neighbour(way):
        return device(z, y, xr if way == 0 else xl, s)

    below, above = div(rem(y + 3, 4), 2), div(rem(y + 1, 4), 2)

    def half_of(first, way, half):
        return pl.ds(pl.multiple_of(first + 32 * rem(way + half, 2), 32), 32)

    def y_move(t, half):
        g, first = rows_of(t)
        for way, target in ((0, y_up), (1, y_down)):
            block = orb.at[own, half_of(first, way, half)]
            send(block, block, y_send, y_recv.at[way, g, half], target)

    def pass_own(t, carry):
        g, first = rows_of(t)
        arrived(t, g)
        y_move(t, 0)

        @pl.when(t < EAGER)
        def _():
            y_move(t, 1)

        block = orb.at[own, pl.ds(first, 64)]
        send(block, orb.at[2, pl.ds(first, 64)], d_send, d_recv, sibling)
        return carry

    def y_wait(t, half):
        g, _ = rows_of(t)
        for way in range(2):
            drain(app.at[pl.ds(0, 32)], y_recv.at[way, g, half])

    def pass_others(t):
        g, first = rows_of(t)
        for way, plane, target in ((0, below, y_up), (1, above, y_down)):
            drain(app.at[pl.ds(0, 32)], y_recv.at[way, g, 0])
            block = orb.at[plane, half_of(first, way, 0)]
            send(block, block, y_send, y_recv.at[way, g, 0], target)

    def hand_over(t):
        g, first = rows_of(t)
        arrived(t, g)
        piece = app.at[pl.ds(first, 64)]
        send(piece, piece, d_send, d_recv, sibling)

    def set_left(t):
        _, first = rows_of(t)
        for q in range(2):
            to = pl.ds(pl.multiple_of((t * 2 + q) * 64, 64), 64)
            for k, piece in enumerate(split3(orb[q, pl.ds(first, 64), :], 1)):
                left[to, k * DEPTH : (k + 1) * DEPTH] = piece

    def set_right(read):
        def step(n, carry):
            at = pl.ds(pl.multiple_of(n * 64, 64), 64)
            for k, piece in enumerate(split3(read(at), 2)):
                right[at, k * DEPTH : (k + 1) * DEPTH] = piece
            return carry

        lax.fori_loop(0, 8, step, 0)

    def multiply(mat, p):
        got = lax.dot_general(
            left[pl.ds(pl.multiple_of(p * 256, 256), 256), :], right[...],
            (((1,), (1,)), ((), ())), preferred_element_type=jnp.float32,
        )
        for n in range(4):
            t, q = p * 2 + n // 2, n % 2
            _, zl_t, _ = place(t, q)
            for c in range(4):
                e = c if mat else rem(c + 8 - zl_t - turn_of(plane_of(q)), 4)
                part[mat * 16 + p * 4 + n, e] = got[
                    n * 64 : (n + 1) * 64, c * 128 : (c + 1) * 128
                ]

    def place(t, q):
        zz = rem(z + offset_at(t), 8)
        zl_t = rem(zz, 4)
        return rem(2 * rem(zl_t, 2) + q + 4 - x, 4), zl_t, div(zz, 4)

    def spans(mat, q):
        if mat:
            return ((True, 4),)
        whole = plane_of(q) == 0
        return ((whole, 4), (jnp.logical_not(whole), 2))

    def x_move(mat, n, way, count, half):
        some = (n, pl.ds(0, count), pl.ds(32 * half, 32))
        send(
            part.at[some], xbuf.at[(way,) + some], x_send.at[mat],
            x_recv.at[way, n], neighbour(way),
        )

    def x_wait(n, way, count, first, rows):
        drain(
            xbuf.at[way, n, pl.ds(0, count), pl.ds(first, rows)], x_recv.at[way, n]
        )

    def pieces(mat, t, action):
        for q in range(2):
            n = mat * 16 + t * 2 + q
            far, zl_t, r = place(t, q)
            for cond, count in spans(mat, q):
                action(n, q, far, zl_t, r, cond, count)

    def x_first(mat, t):
        def action(n, q, far, zl_t, r, cond, count):
            @pl.when(cond & (far == 2))
            def _():
                for way in range(2):
                    x_move(mat, n, way, count, way)

            for way, near in ((0, 1), (1, 3)):

                @pl.when(cond & (far == near))
                def _(way=way):
                    x_move(mat, n, way, count, 1 - way)

        pieces(mat, t, action)

    def x_second(mat, t):
        def action(n, q, far, zl_t, r, cond, count):
            for way, near in ((0, 1), (1, 3)):

                @pl.when(cond & (far == near))
                def _(way=way):
                    x_wait(n, way, count, 32 * way, 32)
                    some = (n, pl.ds(0, count), pl.ds(32 * way, 32))
                    part[some] = part[some] + xbuf[(way,) + some]
                    x_move(mat, n, way, count, way)

        pieces(mat, t, action)

    def x_last(mat, t):
        def action(n, q, far, zl_t, r, cond, count):
            @pl.when(cond & (far == 0))
            def _():
                x_wait(n, 0, count, 0, 64)
                x_wait(n, 1, count, 0, 64)
                half = pl.ds(pl.multiple_of(r * 64, 64), 64)
                for e in range(count):
                    c = e if mat else rem(zl_t + turn_of(plane_of(q)) + e, 4)
                    zz = div(zl_t, 2) * 4 + c
                    red[mat, zz, half] = part[n, e] + (xbuf[0, n, e] + xbuf[1, n, e])

                    @pl.when(zz != z)
                    def _(zz=zz):
                        send(
                            red.at[mat, zz, half],
                            zbuf.at[mat, rem(z - zz + 8, 8) - 1, half],
                            z_send.at[mat], z_recv.at[mat], device(zz, y, x, s),
                        )

        pieces(mat, t, action)

    def z_sum(mat):
        drain(zbuf.at[mat], z_recv.at[mat])
        total = red[mat, z]
        for n in range(7):
            total = total + zbuf[mat, n]
        return total

    def pair(p, action):
        action(2 * p)
        action(2 * p + 1)

    @pl.when(role_a)
    def _():
        lax.fori_loop(0, 8, pass_own, 0)

        def rest(t, carry):
            y_move(t, 1)
            return carry

        lax.fori_loop(EAGER, 8, rest, 0)

    @pl.when(role_b)
    def _():
        def step(t, carry):
            pass_others(t)
            return carry

        lax.fori_loop(0, 4, step, 0)
        drain(app, d_recv)

    mine_at = jnp.where(role_a, own, 2)
    set_right(lambda at: orb[mine_at, at, :])

    def overlaps(p, carry):
        @pl.when(role_a)
        def _():
            pair(p, lambda t: y_wait(t, 0))

        @pl.when(role_b & (p < 2))
        def _():
            pair(p + 2, pass_others)

        @pl.when(role_b)
        def _():
            pair(p, lambda t: y_wait(t, 1))

        pair(p, set_left)
        multiply(0, p)
        pair(p, lambda t: x_first(0, t))

        @pl.when(p >= 1)
        def _():
            pair(p - 1, lambda t: x_second(0, t))

        @pl.when(role_b & (p >= 1))
        def _():
            pair(p - 1, hand_over)

        return carry

    lax.fori_loop(0, 4, overlaps, 0)

    @pl.when(role_b)
    def _():
        pair(3, hand_over)

    @pl.when(role_a)
    def _():
        drain(app, d_recv)

    set_right(lambda at: app[at, :])

    def energies(p, carry):
        multiply(1, p)

        @pl.when(p < 2)
        def _():
            pair(p, lambda t: x_first(1, t))

        @pl.when(p == 0)
        def _():
            pair(3, lambda t: x_second(0, t))

        return carry

    lax.fori_loop(0, 4, energies, 0)
    pair(0, lambda t: x_last(0, t))
    pair(1, lambda t: x_last(0, t))
    pair(0, lambda t: x_second(1, t))
    pair(2, lambda t: x_first(1, t))
    pair(2, lambda t: x_last(0, t))
    pair(1, lambda t: x_second(1, t))
    pair(3, lambda t: x_first(1, t))
    pair(3, lambda t: x_last(0, t))
    pair(2, lambda t: x_second(1, t))
    pair(0, lambda t: x_last(1, t))
    pair(1, lambda t: x_last(1, t))
    pair(3, lambda t: x_second(1, t))
    pair(2, lambda t: x_last(1, t))

    @pl.when(summed)
    def _():
        total = z_sum(0)
        ovl_ref[...] = total

        @pl.when(row_plane != 0)
        def _():
            turned[0] = total.T
            send(turned.at[0], turned.at[1], t_send, t_recv, mirror)

    pair(3, lambda t: x_last(1, t))
    ham_ref[...] = z_sum(1)

    @pl.when(jnp.logical_not(summed))
    def _():
        drain(turned.at[1], t_recv)
        ovl_ref[...] = turned[1]

    drain(orb.at[0, pl.ds(0, 504)], a_send)

    @pl.when(role_a)
    def _():
        drain(orb.at[pl.ds(0, 2)], y_send)

    @pl.when(role_b)
    def _():
        drain(orb.at[0], y_send)

    drain(app, d_send)

    def x_done(cond, mat, whole_pieces):
        @pl.when(cond)
        def _():
            drain(xbuf.at[0, pl.ds(0, whole_pieces)], x_send.at[mat])

    x_done(role_b, 0, 6)
    x_done(role_a & (rem(x, 2) == own), 0, 8)
    x_done(role_a & (rem(x, 2) != own), 0, 10)
    x_done(True, 1, 12)

    def z_done(cond, mat, halves):
        @pl.when(cond)
        def _():
            drain(xbuf.at[0, 0:halves, 0], z_send.at[mat])

    z_done(row_plane == 0, 0, 14)
    z_done((row_plane != 0) & summed, 0, 6)
    z_done(jnp.logical_not(summed), 0, 8)
    z_done(True, 1, 14)

    @pl.when(summed & (row_plane != 0))
    def _():
        drain(turned.at[0], t_send)


def shards(orbitals, applied):
    f32, dma = jnp.float32, pltpu.SemaphoreType.DMA
    tile = jax.ShapeDtypeStruct((128, 128), f32)
    ham, ovl = pl.pallas_call(
        kernel,
        out_shape=(tile, tile),
        in_specs=[pl.BlockSpec(memory_space=pl.ANY)] * 2,
        out_specs=(pl.BlockSpec(memory_space=pltpu.VMEM),) * 2,
        scratch_shapes=[
            pltpu.VMEM((2, 8, 28672), f32),
            pltpu.VMEM((3, 512, DEPTH), f32),
            pltpu.VMEM((512, DEPTH), f32),
            pltpu.VMEM((1024, 3 * DEPTH), jnp.bfloat16),
            pltpu.VMEM((512, 3 * DEPTH), jnp.bfloat16),
            pltpu.VMEM((32, 4, 64, 128), f32),
            pltpu.VMEM((2, 32, 4, 64, 128), f32),
            pltpu.VMEM((2, 8, 128, 128), f32),
            pltpu.VMEM((2, 7, 128, 128), f32),
            pltpu.VMEM((2, 128, 128), f32),
            dma((2,)), dma, dma, dma((8,)), dma, dma((2, 8, 2)), dma, dma,
            dma((2,)), dma((2, 32)), dma((2,)), dma((2,)), dma, dma,
        ],
        compiler_params=pltpu.CompilerParams(
            collective_id=0, has_side_effects=True, vmem_limit_bytes=56 * 1024 * 1024
        ),
    )(orbitals, applied)
    return pl.pallas_call(
        settle, out_shape=(tile, tile),
        in_specs=[pl.BlockSpec(memory_space=pltpu.VMEM)] * 2,
        out_specs=(pl.BlockSpec(memory_space=pltpu.VMEM),) * 2,
    )(ham, ovl)


def settle(ham_ref, ovl_ref, ham_out, ovl_out):
    ham_out[...] = ham_ref[...]
    ovl_out[...] = ovl_ref[...]


def solution(mesh):
    placed = (P(("row", "col"), None),) * 2
    out = P("col", "row")
    return jax.shard_map(
        shards, mesh=mesh, in_specs=placed, out_specs=(out, out), check_vma=False
    )
```

```python
import jax
import jax.numpy as jnp
from jax import lax
from jax.experimental import pallas as pl
from jax.experimental.pallas import tpu as pltpu
from jax.sharding import PartitionSpec as P

MESH = pl.DeviceIdType.MESH
DEPTH = 896
EAGER = 5
div, rem = lax.div, lax.rem


def drain(ref, sem):
    pltpu.make_async_copy(ref, ref, sem).wait()


def offset_at(t):
    odd = rem(t, 2)
    return odd * div(t + 1, 2) + (1 - odd) * rem(8 - div(t, 2), 8)


def split3(value, low_at):
    hi = value.astype(jnp.bfloat16)
    lo = (value - hi.astype(jnp.float32)).astype(jnp.bfloat16)
    return [lo if n == low_at else hi for n in range(3)]


def kernel(
    orb_hbm, app_hbm, ham_ref, ovl_ref,
    inp, orb, app, left, right, part, xbuf, red, zbuf, turned,
    in_sem, loc_sem, a_send, a_recv, y_send, y_recv, d_send, d_recv,
    x_send, x_recv, z_send, z_recv, t_send, t_recv,
):
    row, col = lax.axis_index("row"), lax.axis_index("col")
    zl, y = div(row, 4), rem(row, 4)
    zh, x, s = div(col, 8), rem(div(col, 2), 4), rem(col, 2)
    z = zh * 4 + zl
    giver = rem(y, 2)
    role_a = s == giver
    role_b = s != giver
    own = div(y, 2)

    def turn_of(plane):
        return jnp.where((plane == 3) | ((plane == 2) & (y >= 2)), 1, 0)

    def plane_of(q):
        return rem(s + 2 * q + 4 - y, 4)

    row_plane = plane_of(rem(x, 2))
    tile_at = rem(zl + 8 - (2 * zh + div(x, 2)) - turn_of(row_plane), 4)
    summed = (row_plane == 0) | (tile_at < 2)
    mirror = (col, row)

    def device(zz, yy, xx, ss):
        return (rem(zz, 4) * 4 + yy, div(zz, 4) * 8 + xx * 2 + ss)

    def send(src, dst, send_sem, recv_sem, target):
        pltpu.make_async_remote_copy(
            src_ref=src, dst_ref=dst, send_sem=send_sem, recv_sem=recv_sem,
            device_id=target, device_id_type=MESH,
        ).start()

    sibling = device(z, y, x, 1 - s)
    y_up, y_down = device(z, rem(y + 1, 4), x, s), device(z, rem(y + 3, 4), x, s)
    xr, xl = rem(x + 1, 4), rem(x + 3, 4)

    loads = [
        pltpu.make_async_copy(orb_hbm, inp.at[0], in_sem.at[0]),
        pltpu.make_async_copy(app_hbm, inp.at[1], in_sem.at[1]),
    ]
    for load in loads:
        load.start()

    barrier = pltpu.get_barrier_semaphore()

    def greet(n, carry):
        zz = rem(z + offset_at(7 - n), 8)
        for i in range(8):
            pl.semaphore_signal(
                barrier, inc=1, device_id=(rem(zz, 4) * 4 + y, div(zz, 4) * 8 + i),
                device_id_type=MESH,
            )
        return carry

    @pl.when(row_plane != 0)
    def _():
        pl.semaphore_signal(barrier, inc=1, device_id=mirror, device_id_type=MESH)

    lax.fori_loop(0, 7, greet, 0)
    for i in range(1, 8):
        pl.semaphore_signal(
            barrier, inc=1, device_id=(row, zh * 8 + rem(x * 2 + s + i, 8)),
            device_id_type=MESH,
        )
    for target in (y_up, y_down):
        pl.semaphore_signal(barrier, inc=1, device_id=target, device_id_type=MESH)
    for load in loads:
        load.wait()
    pl.semaphore_wait(barrier, jnp.where(row_plane == 0, 65, 66))

    slot = pl.ds(pl.multiple_of(zl * 128 + col * 8, 8), 8)
    orb_slot, app_slot = orb.at[own, slot], app.at[slot]

    def columns(zz, xx):
        return pl.ds(pl.multiple_of((zz * 4 + xx) * DEPTH, 128), DEPTH)

    def scatter(which, dst, core):
        def step(n, carry):
            d = offset_at(div(n, 4))
            zz, xx = rem(z + d, 8), rem(x + rem(n, 4), 4)
            send(
                inp.at[which, :, columns(zz, xx)], dst, a_send,
                a_recv.at[rem(8 - d, 8)], device(zz, y, xx, core),
            )
            return carry

        lax.fori_loop(1, 32, step, 0)

    orb_mine, app_mine = inp.at[0, :, columns(z, x)], inp.at[1, :, columns(z, x)]

    @pl.when(role_a)
    def _():
        pltpu.make_async_copy(orb_mine, orb_slot, loc_sem).start()

    @pl.when(role_b)
    def _():
        send(orb_mine, orb_slot, a_send, a_recv.at[0], sibling)

    scatter(0, orb_slot, giver)

    @pl.when(role_a)
    def _():
        send(app_mine, app_slot, a_send, a_recv.at[0], sibling)

    @pl.when(role_b)
    def _():
        pltpu.make_async_copy(app_mine, app_slot, loc_sem).start()

    scatter(1, app_slot, 1 - giver)

    def rows_of(t):
        g = offset_at(t)
        zz = rem(z + g, 8)
        return g, pl.multiple_of(rem(zz, 4) * 128 + div(zz, 4) * 64, 64)

    def arrived(t, g):
        @pl.when(t == 0)
        def _():
            drain(app.at[pl.ds(0, 56)], a_recv.at[0])
            drain(app.at[pl.ds(0, 8)], loc_sem)

        @pl.when(t > 0)
        def _():
            drain(app.at[pl.ds(0, 64)], a_recv.at[g])

    def neighbour(way):
        return device(z, y, xr if way == 0 else xl, s)

    below, above = div(rem(y + 3, 4), 2), div(rem(y + 1, 4), 2)

    def half_of(first, way, half):
        return pl.ds(pl.multiple_of(first + 32 * rem(way + half, 2), 32), 32)

    def y_move(t, half):
        g, first = rows_of(t)
        for way, target in ((0, y_up), (1, y_down)):
            block = orb.at[own, half_of(first, way, half)]
            send(block, block, y_send, y_recv.at[way, g, half], target)

    def pass_own(t, carry):
        g, first = rows_of(t)
        arrived(t, g)
        y_move(t, 0)

        @pl.when(t < EAGER)
        def _():
            y_move(t, 1)

        block = orb.at[own, pl.ds(first, 64)]
        send(block, orb.at[2, pl.ds(first, 64)], d_send, d_recv, sibling)
        return carry

    def y_wait(t, half):
        g, _ = rows_of(t)
        for way in range(2):
            drain(app.at[pl.ds(0, 32)], y_recv.at[way, g, half])

    def pass_others(t):
        g, first = rows_of(t)
        for way, plane, target in ((0, below, y_up), (1, above, y_down)):
            drain(app.at[pl.ds(0, 32)], y_recv.at[way, g, 0])
            block = orb.at[plane, half_of(first, way, 0)]
            send(block, block, y_send, y_recv.at[way, g, 0], target)

    def hand_over(t):
        g, first = rows_of(t)
        arrived(t, g)
        piece = app.at[pl.ds(first, 64)]
        send(piece, piece, d_send, d_recv, sibling)

    def set_left(t):
        _, first = rows_of(t)
        for q in range(2):
            to = pl.ds(pl.multiple_of((t * 2 + q) * 64, 64), 64)
            for k, piece in enumerate(split3(orb[q, pl.ds(first, 64), :], 1)):
                left[to, k * DEPTH : (k + 1) * DEPTH] = piece

    def set_right(read):
        def step(n, carry):
            at = pl.ds(pl.multiple_of(n * 64, 64), 64)
            for k, piece in enumerate(split3(read(at), 2)):
                right[at, k * DEPTH : (k + 1) * DEPTH] = piece
            return carry

        lax.fori_loop(0, 8, step, 0)

    def multiply(mat, p):
        got = lax.dot_general(
            left[pl.ds(pl.multiple_of(p * 256, 256), 256), :], right[...],
            (((1,), (1,)), ((), ())), preferred_element_type=jnp.float32,
        )
        for n in range(4):
            t, q = p * 2 + n // 2, n % 2
            _, zl_t, _ = place(t, q)
            for c in range(4):
                e = c if mat else rem(c + 8 - zl_t - turn_of(plane_of(q)), 4)
                part[mat * 16 + p * 4 + n, e] = got[
                    n * 64 : (n + 1) * 64, c * 128 : (c + 1) * 128
                ]

    def place(t, q):
        zz = rem(z + offset_at(t), 8)
        zl_t = rem(zz, 4)
        return rem(2 * rem(zl_t, 2) + q + 4 - x, 4), zl_t, div(zz, 4)

    def spans(mat, q):
        if mat:
            return ((True, 4),)
        whole = plane_of(q) == 0
        return ((whole, 4), (jnp.logical_not(whole), 2))

    def x_move(mat, n, way, count, half):
        some = (n, pl.ds(0, count), pl.ds(32 * half, 32))
        send(
            part.at[some], xbuf.at[(way,) + some], x_send.at[mat],
            x_recv.at[way, n], neighbour(way),
        )

    def x_wait(n, way, count, first, rows):
        drain(
            xbuf.at[way, n, pl.ds(0, count), pl.ds(first, rows)], x_recv.at[way, n]
        )

    def pieces(mat, t, action):
        for q in range(2):
            n = mat * 16 + t * 2 + q
            far, zl_t, r = place(t, q)
            for cond, count in spans(mat, q):
                action(n, q, far, zl_t, r, cond, count)

    def x_first(mat, t):
        def action(n, q, far, zl_t, r, cond, count):
            @pl.when(cond & (far == 2))
            def _():
                for way in range(2):
                    x_move(mat, n, way, count, way)

            for way, near in ((0, 1), (1, 3)):

                @pl.when(cond & (far == near))
                def _(way=way):
                    x_move(mat, n, way, count, 1 - way)

        pieces(mat, t, action)

    def x_second(mat, t):
        def action(n, q, far, zl_t, r, cond, count):
            for way, near in ((0, 1), (1, 3)):

                @pl.when(cond & (far == near))
                def _(way=way):
                    x_wait(n, way, count, 32 * way, 32)
                    some = (n, pl.ds(0, count), pl.ds(32 * way, 32))
                    part[some] = part[some] + xbuf[(way,) + some]
                    x_move(mat, n, way, count, way)

        pieces(mat, t, action)

    def x_last(mat, t):
        def action(n, q, far, zl_t, r, cond, count):
            @pl.when(cond & (far == 0))
            def _():
                x_wait(n, 0, count, 0, 64)
                x_wait(n, 1, count, 0, 64)
                half = pl.ds(pl.multiple_of(r * 64, 64), 64)
                for e in range(count):
                    c = e if mat else rem(zl_t + turn_of(plane_of(q)) + e, 4)
                    zz = div(zl_t, 2) * 4 + c
                    red[mat, zz, half] = part[n, e] + (xbuf[0, n, e] + xbuf[1, n, e])

                    @pl.when(zz != z)
                    def _(zz=zz):
                        send(
                            red.at[mat, zz, half],
                            zbuf.at[mat, rem(z - zz + 8, 8) - 1, half],
                            z_send.at[mat], z_recv.at[mat], device(zz, y, x, s),
                        )

        pieces(mat, t, action)

    def z_sum(mat):
        drain(zbuf.at[mat], z_recv.at[mat])
        total = red[mat, z]
        for n in range(7):
            total = total + zbuf[mat, n]
        return total

    def pair(p, action):
        action(2 * p)
        action(2 * p + 1)

    @pl.when(role_a)
    def _():
        lax.fori_loop(0, 8, pass_own, 0)

        def rest(t, carry):
            y_move(t, 1)
            return carry

        lax.fori_loop(EAGER, 8, rest, 0)

    @pl.when(role_b)
    def _():
        def step(t, carry):
            pass_others(t)
            return carry

        lax.fori_loop(0, 4, step, 0)
        drain(app, d_recv)

    mine_at = jnp.where(role_a, own, 2)
    set_right(lambda at: orb[mine_at, at, :])

    def overlaps(p, carry):
        @pl.when(role_a)
        def _():
            pair(p, lambda t: y_wait(t, 0))

        @pl.when(role_b & (p < 2))
        def _():
            pair(p + 2, pass_others)

        @pl.when(role_b)
        def _():
            pair(p, lambda t: y_wait(t, 1))

        pair(p, set_left)
        multiply(0, p)
        pair(p, lambda t: x_first(0, t))

        @pl.when(p >= 1)
        def _():
            pair(p - 1, lambda t: x_second(0, t))

        @pl.when(role_b & (p >= 1))
        def _():
            pair(p - 1, hand_over)

        return carry

    lax.fori_loop(0, 4, overlaps, 0)

    @pl.when(role_b)
    def _():
        pair(3, hand_over)

    @pl.when(role_a)
    def _():
        drain(app, d_recv)

    set_right(lambda at: app[at, :])

    def energies(p, carry):
        multiply(1, p)

        @pl.when(p < 2)
        def _():
            pair(p, lambda t: x_first(1, t))

        @pl.when(p == 0)
        def _():
            pair(3, lambda t: x_second(0, t))

        return carry

    lax.fori_loop(0, 4, energies, 0)
    pair(0, lambda t: x_last(0, t))
    pair(1, lambda t: x_last(0, t))
    pair(0, lambda t: x_second(1, t))
    pair(2, lambda t: x_first(1, t))
    pair(2, lambda t: x_last(0, t))
    pair(1, lambda t: x_second(1, t))
    pair(3, lambda t: x_first(1, t))
    pair(3, lambda t: x_last(0, t))
    pair(2, lambda t: x_second(1, t))
    pair(0, lambda t: x_last(1, t))
    pair(1, lambda t: x_last(1, t))
    pair(2, lambda t: x_last(1, t))
    pair(3, lambda t: x_second(1, t))

    @pl.when(summed)
    def _():
        total = z_sum(0)
        ovl_ref[...] = total

        @pl.when(row_plane != 0)
        def _():
            turned[0] = total.T
            send(turned.at[0], turned.at[1], t_send, t_recv, mirror)

    pair(3, lambda t: x_last(1, t))
    ham_ref[...] = z_sum(1)

    @pl.when(jnp.logical_not(summed))
    def _():
        drain(turned.at[1], t_recv)
        ovl_ref[...] = turned[1]

    drain(orb.at[0, pl.ds(0, 504)], a_send)

    @pl.when(role_a)
    def _():
        drain(orb.at[pl.ds(0, 2)], y_send)

    @pl.when(role_b)
    def _():
        drain(orb.at[0], y_send)

    drain(app, d_send)

    def x_done(cond, mat, whole_pieces):
        @pl.when(cond)
        def _():
            drain(xbuf.at[0, pl.ds(0, whole_pieces)], x_send.at[mat])

    x_done(role_b, 0, 6)
    x_done(role_a & (rem(x, 2) == own), 0, 8)
    x_done(role_a & (rem(x, 2) != own), 0, 10)
    x_done(True, 1, 12)

    def z_done(cond, mat, halves):
        @pl.when(cond)
        def _():
            drain(xbuf.at[0, 0:halves, 0], z_send.at[mat])

    z_done(row_plane == 0, 0, 14)
    z_done((row_plane != 0) & summed, 0, 6)
    z_done(jnp.logical_not(summed), 0, 8)
    z_done(True, 1, 14)

    @pl.when(summed & (row_plane != 0))
    def _():
        drain(turned.at[0], t_send)


def shards(orbitals, applied):
    f32, dma = jnp.float32, pltpu.SemaphoreType.DMA
    tile = jax.ShapeDtypeStruct((128, 128), f32)
    ham, ovl = pl.pallas_call(
        kernel,
        out_shape=(tile, tile),
        in_specs=[pl.BlockSpec(memory_space=pl.ANY)] * 2,
        out_specs=(pl.BlockSpec(memory_space=pltpu.VMEM),) * 2,
        scratch_shapes=[
            pltpu.VMEM((2, 8, 28672), f32),
            pltpu.VMEM((3, 512, DEPTH), f32),
            pltpu.VMEM((512, DEPTH), f32),
            pltpu.VMEM((1024, 3 * DEPTH), jnp.bfloat16),
            pltpu.VMEM((512, 3 * DEPTH), jnp.bfloat16),
            pltpu.VMEM((32, 4, 64, 128), f32),
            pltpu.VMEM((2, 32, 4, 64, 128), f32),
            pltpu.VMEM((2, 8, 128, 128), f32),
            pltpu.VMEM((2, 7, 128, 128), f32),
            pltpu.VMEM((2, 128, 128), f32),
            dma((2,)), dma, dma, dma((8,)), dma, dma((2, 8, 2)), dma, dma,
            dma((2,)), dma((2, 32)), dma((2,)), dma((2,)), dma, dma,
        ],
        compiler_params=pltpu.CompilerParams(
            collective_id=0, has_side_effects=True, vmem_limit_bytes=56 * 1024 * 1024
        ),
    )(orbitals, applied)
    return pl.pallas_call(
        settle, out_shape=(tile, tile),
        in_specs=[pl.BlockSpec(memory_space=pltpu.VMEM)] * 2,
        out_specs=(pl.BlockSpec(memory_space=pltpu.VMEM),) * 2,
    )(ham, ovl)


def settle(ham_ref, ovl_ref, ham_out, ovl_out):
    ham_out[...] = ham_ref[...]
    ovl_out[...] = ovl_ref[...]


def solution(mesh):
    placed = (P(("row", "col"), None),) * 2
    out = P("col", "row")
    return jax.shard_map(
        shards, mesh=mesh, in_specs=placed, out_specs=(out, out), check_vma=False
    )
```

```python
import jax
import jax.numpy as jnp
from jax import lax
from jax.experimental import pallas as pl
from jax.experimental.pallas import tpu as pltpu
from jax.sharding import PartitionSpec as P

MESH = pl.DeviceIdType.MESH
DEPTH = 896
EAGER = 5
div, rem = lax.div, lax.rem


def drain(ref, sem):
    pltpu.make_async_copy(ref, ref, sem).wait()


def offset_at(t):
    odd = rem(t, 2)
    return odd * div(t + 1, 2) + (1 - odd) * rem(8 - div(t, 2), 8)


def split3(value, low_at):
    hi = value.astype(jnp.bfloat16)
    lo = (value - hi.astype(jnp.float32)).astype(jnp.bfloat16)
    return [lo if n == low_at else hi for n in range(3)]


def kernel(
    orb_hbm, app_hbm, ham_ref, ovl_ref,
    inp, orb, app, left, right, part, xbuf, red, zbuf, turned,
    in_sem, loc_sem, a_send, a_recv, y_send, y_recv, d_send, d_recv,
    x_send, x_recv, z_send, z_recv, t_send, t_recv,
):
    row, col = lax.axis_index("row"), lax.axis_index("col")
    zl, y = div(row, 4), rem(row, 4)
    zh, x, s = div(col, 8), rem(div(col, 2), 4), rem(col, 2)
    z = zh * 4 + zl
    giver = rem(y, 2)
    role_a = s == giver
    role_b = s != giver
    own = div(y, 2)

    def turn_of(plane):
        return jnp.where((plane == 3) | ((plane == 2) & (y >= 2)), 1, 0)

    def plane_of(q):
        return rem(s + 2 * q + 4 - y, 4)

    row_plane = plane_of(rem(x, 2))
    tile_at = rem(zl + 8 - (2 * zh + div(x, 2)) - turn_of(row_plane), 4)
    summed = (row_plane == 0) | (tile_at < 2)
    mirror = (col, row)

    def device(zz, yy, xx, ss):
        return (rem(zz, 4) * 4 + yy, div(zz, 4) * 8 + xx * 2 + ss)

    def send(src, dst, send_sem, recv_sem, target):
        pltpu.make_async_remote_copy(
            src_ref=src, dst_ref=dst, send_sem=send_sem, recv_sem=recv_sem,
            device_id=target, device_id_type=MESH,
        ).start()

    sibling = device(z, y, x, 1 - s)
    y_up, y_down = device(z, rem(y + 1, 4), x, s), device(z, rem(y + 3, 4), x, s)
    xr, xl = rem(x + 1, 4), rem(x + 3, 4)

    loads = [
        pltpu.make_async_copy(orb_hbm, inp.at[0], in_sem.at[0]),
        pltpu.make_async_copy(app_hbm, inp.at[1], in_sem.at[1]),
    ]
    for load in loads:
        load.start()

    barrier = pltpu.get_barrier_semaphore()

    def greet(n, carry):
        zz = rem(z + offset_at(7 - n), 8)
        for i in range(8):
            pl.semaphore_signal(
                barrier, inc=1, device_id=(rem(zz, 4) * 4 + y, div(zz, 4) * 8 + i),
                device_id_type=MESH,
            )
        return carry

    @pl.when(row_plane != 0)
    def _():
        pl.semaphore_signal(barrier, inc=1, device_id=mirror, device_id_type=MESH)

    lax.fori_loop(0, 7, greet, 0)
    for i in range(1, 8):
        pl.semaphore_signal(
            barrier, inc=1, device_id=(row, zh * 8 + rem(x * 2 + s + i, 8)),
            device_id_type=MESH,
        )
    for target in (y_up, y_down):
        pl.semaphore_signal(barrier, inc=1, device_id=target, device_id_type=MESH)
    for load in loads:
        load.wait()
    pl.semaphore_wait(barrier, jnp.where(row_plane == 0, 65, 66))

    slot = pl.ds(pl.multiple_of(zl * 128 + col * 8, 8), 8)
    orb_slot, app_slot = orb.at[own, slot], app.at[slot]

    def columns(zz, xx):
        return pl.ds(pl.multiple_of((zz * 4 + xx) * DEPTH, 128), DEPTH)

    def scatter(which, dst, core):
        def step(n, carry):
            d = offset_at(div(n, 4))
            zz, xx = rem(z + d, 8), rem(x + rem(n, 4), 4)
            send(
                inp.at[which, :, columns(zz, xx)], dst, a_send,
                a_recv.at[rem(8 - d, 8)], device(zz, y, xx, core),
            )
            return carry

        lax.fori_loop(1, 32, step, 0)

    orb_mine, app_mine = inp.at[0, :, columns(z, x)], inp.at[1, :, columns(z, x)]

    @pl.when(role_a)
    def _():
        pltpu.make_async_copy(orb_mine, orb_slot, loc_sem).start()

    @pl.when(role_b)
    def _():
        send(orb_mine, orb_slot, a_send, a_recv.at[0], sibling)

    scatter(0, orb_slot, giver)

    @pl.when(role_a)
    def _():
        send(app_mine, app_slot, a_send, a_recv.at[0], sibling)

    @pl.when(role_b)
    def _():
        pltpu.make_async_copy(app_mine, app_slot, loc_sem).start()

    scatter(1, app_slot, 1 - giver)

    def rows_of(t):
        g = offset_at(t)
        zz = rem(z + g, 8)
        return g, pl.multiple_of(rem(zz, 4) * 128 + div(zz, 4) * 64, 64)

    def arrived(t, g):
        @pl.when(t == 0)
        def _():
            drain(app.at[pl.ds(0, 56)], a_recv.at[0])
            drain(app.at[pl.ds(0, 8)], loc_sem)

        @pl.when(t > 0)
        def _():
            drain(app.at[pl.ds(0, 64)], a_recv.at[g])

    def neighbour(way):
        return device(z, y, xr if way == 0 else xl, s)

    below, above = div(rem(y + 3, 4), 2), div(rem(y + 1, 4), 2)

    def half_of(first, way, half):
        return pl.ds(pl.multiple_of(first + 32 * rem(way + half, 2), 32), 32)

    def y_move(t, half):
        g, first = rows_of(t)
        for way, target in ((0, y_up), (1, y_down)):
            block = orb.at[own, half_of(first, way, half)]
            send(block, block, y_send, y_recv.at[way, g, half], target)

    def pass_own(t, carry):
        g, first = rows_of(t)
        arrived(t, g)
        y_move(t, 0)

        @pl.when(t < EAGER)
        def _():
            y_move(t, 1)

        block = orb.at[own, pl.ds(first, 64)]
        send(block, orb.at[2, pl.ds(first, 64)], d_send, d_recv, sibling)
        return carry

    def y_wait(t, half):
        g, _ = rows_of(t)
        for way in range(2):
            drain(app.at[pl.ds(0, 32)], y_recv.at[way, g, half])

    def pass_others(t):
        g, first = rows_of(t)
        for way, plane, target in ((0, below, y_up), (1, above, y_down)):
            drain(app.at[pl.ds(0, 32)], y_recv.at[way, g, 0])
            block = orb.at[plane, half_of(first, way, 0)]
            send(block, block, y_send, y_recv.at[way, g, 0], target)

    def hand_over(t):
        g, first = rows_of(t)
        arrived(t, g)
        piece = app.at[pl.ds(first, 64)]
        send(piece, piece, d_send, d_recv, sibling)

    def set_left(t):
        _, first = rows_of(t)
        for q in range(2):
            to = pl.ds(pl.multiple_of((t * 2 + q) * 64, 64), 64)
            for k, piece in enumerate(split3(orb[q, pl.ds(first, 64), :], 1)):
                left[to, k * DEPTH : (k + 1) * DEPTH] = piece

    def set_right(read):
        def step(n, carry):
            at = pl.ds(pl.multiple_of(n * 64, 64), 64)
            for k, piece in enumerate(split3(read(at), 2)):
                right[at, k * DEPTH : (k + 1) * DEPTH] = piece
            return carry

        lax.fori_loop(0, 8, step, 0)

    def multiply(mat, p):
        got = lax.dot_general(
            left[pl.ds(pl.multiple_of(p * 256, 256), 256), :], right[...],
            (((1,), (1,)), ((), ())), preferred_element_type=jnp.float32,
        )
        for n in range(4):
            t, q = p * 2 + n // 2, n % 2
            _, zl_t, _ = place(t, q)
            for c in range(4):
                e = c if mat else rem(c + 8 - zl_t - turn_of(plane_of(q)), 4)
                part[mat * 16 + p * 4 + n, e] = got[
                    n * 64 : (n + 1) * 64, c * 128 : (c + 1) * 128
                ]

    def place(t, q):
        zz = rem(z + offset_at(t), 8)
        zl_t = rem(zz, 4)
        return rem(2 * rem(zl_t, 2) + q + 4 - x, 4), zl_t, div(zz, 4)

    def spans(mat, q):
        if mat:
            return ((True, 4),)
        whole = plane_of(q) == 0
        return ((whole, 4), (jnp.logical_not(whole), 2))

    def x_move(mat, n, way, count, half):
        some = (n, pl.ds(0, count), pl.ds(32 * half, 32))
        send(
            part.at[some], xbuf.at[(way,) + some], x_send.at[mat],
            x_recv.at[way, n], neighbour(way),
        )

    def x_wait(n, way, count, first, rows):
        drain(
            xbuf.at[way, n, pl.ds(0, count), pl.ds(first, rows)], x_recv.at[way, n]
        )

    def pieces(mat, t, action):
        for q in range(2):
            n = mat * 16 + t * 2 + q
            far, zl_t, r = place(t, q)
            for cond, count in spans(mat, q):
                action(n, q, far, zl_t, r, cond, count)

    def x_first(mat, t):
        def action(n, q, far, zl_t, r, cond, count):
            @pl.when(cond & (far == 2))
            def _():
                for way in range(2):
                    x_move(mat, n, way, count, way)

            for way, near in ((0, 1), (1, 3)):

                @pl.when(cond & (far == near))
                def _(way=way):
                    x_move(mat, n, way, count, 1 - way)

        pieces(mat, t, action)

    def x_second(mat, t):
        def action(n, q, far, zl_t, r, cond, count):
            for way, near in ((0, 1), (1, 3)):

                @pl.when(cond & (far == near))
                def _(way=way):
                    x_wait(n, way, count, 32 * way, 32)
                    some = (n, pl.ds(0, count), pl.ds(32 * way, 32))
                    part[some] = part[some] + xbuf[(way,) + some]
                    x_move(mat, n, way, count, way)

        pieces(mat, t, action)

    def x_last(mat, t):
        def action(n, q, far, zl_t, r, cond, count):
            @pl.when(cond & (far == 0))
            def _():
                x_wait(n, 0, count, 0, 64)
                x_wait(n, 1, count, 0, 64)
                half = pl.ds(pl.multiple_of(r * 64, 64), 64)
                for e in range(count):
                    c = e if mat else rem(zl_t + turn_of(plane_of(q)) + e, 4)
                    zz = div(zl_t, 2) * 4 + c
                    red[mat, zz, half] = part[n, e] + (xbuf[0, n, e] + xbuf[1, n, e])

                    @pl.when(zz != z)
                    def _(zz=zz):
                        send(
                            red.at[mat, zz, half],
                            zbuf.at[mat, rem(z - zz + 8, 8) - 1, half],
                            z_send.at[mat], z_recv.at[mat], device(zz, y, x, s),
                        )

        pieces(mat, t, action)

    def z_sum(mat):
        drain(zbuf.at[mat], z_recv.at[mat])
        total = red[mat, z]
        for n in range(7):
            total = total + zbuf[mat, n]
        return total

    def pair(p, action):
        action(2 * p)
        action(2 * p + 1)

    @pl.when(role_a)
    def _():
        lax.fori_loop(0, 8, pass_own, 0)

        def rest(t, carry):
            y_move(t, 1)
            return carry

        lax.fori_loop(EAGER, 8, rest, 0)

    @pl.when(role_b)
    def _():
        def step(t, carry):
            pass_others(t)
            return carry

        lax.fori_loop(0, 4, step, 0)
        drain(app, d_recv)

    mine_at = jnp.where(role_a, own, 2)
    set_right(lambda at: orb[mine_at, at, :])

    def overlaps(p, carry):
        @pl.when(role_a)
        def _():
            pair(p, lambda t: y_wait(t, 0))

        @pl.when(role_b & (p < 2))
        def _():
            pair(p + 2, pass_others)

        @pl.when(role_b)
        def _():
            pair(p, lambda t: y_wait(t, 1))

        pair(p, set_left)
        multiply(0, p)
        pair(p, lambda t: x_first(0, t))

        @pl.when(p >= 1)
        def _():
            pair(p - 1, lambda t: x_second(0, t))

        @pl.when(role_b & (p >= 1))
        def _():
            pair(p - 1, hand_over)

        return carry

    lax.fori_loop(0, 4, overlaps, 0)

    @pl.when(role_b)
    def _():
        pair(3, hand_over)

    @pl.when(role_a)
    def _():
        drain(app, d_recv)

    set_right(lambda at: app[at, :])

    def energies(p, carry):
        multiply(1, p)

        @pl.when(p < 2)
        def _():
            pair(p, lambda t: x_first(1, t))

        @pl.when(p == 0)
        def _():
            pair(3, lambda t: x_second(0, t))

        return carry

    lax.fori_loop(0, 4, energies, 0)
    pair(0, lambda t: x_last(0, t))
    pair(1, lambda t: x_last(0, t))
    pair(0, lambda t: x_second(1, t))
    pair(2, lambda t: x_first(1, t))
    pair(2, lambda t: x_last(0, t))
    pair(1, lambda t: x_second(1, t))
    pair(3, lambda t: x_first(1, t))
    pair(3, lambda t: x_last(0, t))
    pair(2, lambda t: x_second(1, t))
    pair(0, lambda t: x_last(1, t))
    pair(1, lambda t: x_last(1, t))
    pair(2, lambda t: x_last(1, t))
    pair(3, lambda t: x_second(1, t))

    pair(3, lambda t: x_last(1, t))

    @pl.when(summed)
    def _():
        total = z_sum(0)
        ovl_ref[...] = total

        @pl.when(row_plane != 0)
        def _():
            turned[0] = total.T
            send(turned.at[0], turned.at[1], t_send, t_recv, mirror)

    ham_ref[...] = z_sum(1)

    @pl.when(jnp.logical_not(summed))
    def _():
        drain(turned.at[1], t_recv)
        ovl_ref[...] = turned[1]

    drain(orb.at[0, pl.ds(0, 504)], a_send)

    @pl.when(role_a)
    def _():
        drain(orb.at[pl.ds(0, 2)], y_send)

    @pl.when(role_b)
    def _():
        drain(orb.at[0], y_send)

    drain(app, d_send)

    def x_done(cond, mat, whole_pieces):
        @pl.when(cond)
        def _():
            drain(xbuf.at[0, pl.ds(0, whole_pieces)], x_send.at[mat])

    x_done(role_b, 0, 6)
    x_done(role_a & (rem(x, 2) == own), 0, 8)
    x_done(role_a & (rem(x, 2) != own), 0, 10)
    x_done(True, 1, 12)

    def z_done(cond, mat, halves):
        @pl.when(cond)
        def _():
            drain(xbuf.at[0, 0:halves, 0], z_send.at[mat])

    z_done(row_plane == 0, 0, 14)
    z_done((row_plane != 0) & summed, 0, 6)
    z_done(jnp.logical_not(summed), 0, 8)
    z_done(True, 1, 14)

    @pl.when(summed & (row_plane != 0))
    def _():
        drain(turned.at[0], t_send)


def shards(orbitals, applied):
    f32, dma = jnp.float32, pltpu.SemaphoreType.DMA
    tile = jax.ShapeDtypeStruct((128, 128), f32)
    ham, ovl = pl.pallas_call(
        kernel,
        out_shape=(tile, tile),
        in_specs=[pl.BlockSpec(memory_space=pl.ANY)] * 2,
        out_specs=(pl.BlockSpec(memory_space=pltpu.VMEM),) * 2,
        scratch_shapes=[
            pltpu.VMEM((2, 8, 28672), f32),
            pltpu.VMEM((3, 512, DEPTH), f32),
            pltpu.VMEM((512, DEPTH), f32),
            pltpu.VMEM((1024, 3 * DEPTH), jnp.bfloat16),
            pltpu.VMEM((512, 3 * DEPTH), jnp.bfloat16),
            pltpu.VMEM((32, 4, 64, 128), f32),
            pltpu.VMEM((2, 32, 4, 64, 128), f32),
            pltpu.VMEM((2, 8, 128, 128), f32),
            pltpu.VMEM((2, 7, 128, 128), f32),
            pltpu.VMEM((2, 128, 128), f32),
            dma((2,)), dma, dma, dma((8,)), dma, dma((2, 8, 2)), dma, dma,
            dma((2,)), dma((2, 32)), dma((2,)), dma((2,)), dma, dma,
        ],
        compiler_params=pltpu.CompilerParams(
            collective_id=0, has_side_effects=True, vmem_limit_bytes=56 * 1024 * 1024
        ),
    )(orbitals, applied)
    return pl.pallas_call(
        settle, out_shape=(tile, tile),
        in_specs=[pl.BlockSpec(memory_space=pltpu.VMEM)] * 2,
        out_specs=(pl.BlockSpec(memory_space=pltpu.VMEM),) * 2,
    )(ham, ovl)


def settle(ham_ref, ovl_ref, ham_out, ovl_out):
    ham_out[...] = ham_ref[...]
    ovl_out[...] = ovl_ref[...]


def solution(mesh):
    placed = (P(("row", "col"), None),) * 2
    out = P("col", "row")
    return jax.shard_map(
        shards, mesh=mesh, in_specs=placed, out_specs=(out, out), check_vma=False
    )
```
